256 devices in a mesh: parts: 2 (over y), gz: 32 (over z, core), shot: 4 (over x).
Axes of the slice: x: 4, y: 2, z: 16, core: 2. Of those that a mesh axis runs over, the one named last changes fastest.
The devices are a block of a 4x16x16 slice.
Arguments:
- wavefields: float32 [8, 2, 9, 128, 32, 128], P(('parts', 'shot'), None, None, 'gz'), parts along dimension 0, may hold values from -6 to 6
- earth_model: float32 [6, 128, 32, 128], P('parts', 'gz'), parts along dimension 0, may hold values from 0.4 to 1.6
- source_depth: int32 [8], P(('parts', 'shot')), parts along dimension 0, may hold values from 0 to 127
- source_column: int32 [8], P(('parts', 'shot')), parts along dimension 0, may hold values from 0 to 4095
- wavelet: float32 [8, 8], P(('parts', 'shot')), parts along dimension 0, may hold values from -30 to 30
- receiver_depth: int32 [8, 64], P(('parts', 'shot')), parts along dimension 0, may hold values from 0 to 127
- receiver_column: int32 [8, 64], P(('parts', 'shot')), parts along dimension 0, may hold values from 0 to 4095
- traces: float32 [8, 8, 64], P(('parts', 'shot')), parts along dimension 0, may hold values from -30 to 30
Outputs:
- images: float32 [4, 128, 32, 128], P('parts', 'gz'), parts along dimension 0
The draws below stay inside these ranges and needn't reach their ends.
There are 2 independent parts, one for each index of `parts`. The reference program is written for one: setup_inputs(seed, part) draws one part's arguments, and reference() takes and returns one part's arrays. A program takes and returns all parts, laid end to end along the dimension named above; each array names one. Nothing has to cross between parts.
All inputs are finite; a program needn't handle non-finite values.
Results may differ from the reference program's by a relative error of at most 0.00002.
Values sent between devices are 32-bit elements; how exact they have to be, the bound alone decides.
No kernel may reach another device: no remote copies, remote signals or barrier semaphores. Data moves between devices by JAX's collectives and lax.ppermute only.
A program may use at most 64 MiB of HBM per device.

```python
import math
import jax
import jax.numpy as jnp
from jax import lax

NX = 32
NY = 128
STEPS = 8
RECV = 64
NZ = 128
SHOTS = 4


def plant(drawn, key, smallest, top_value):
    dims = drawn.shape
    spot = [jax.random.randint(jax.random.fold_in(key, axis), (), 0, dims[axis]) for axis in range(len(dims))]
    drawn = drawn.at[tuple(spot)].set(smallest)
    longest = dims.index(max(dims))
    spot[longest] = (spot[longest] + 1) % dims[longest]
    return drawn.at[tuple(spot)].set(top_value)


def levels(stream_key, extent, pieces, least, top_value):
    loudness = 1.0
    for position, parts in pieces:
        heights = jax.random.uniform(jax.random.fold_in(jax.random.fold_in(stream_key, 6), position), (parts,), jnp.float32, least / len(pieces), top_value / len(pieces))
        loudness = loudness * jnp.repeat(jnp.exp(heights), extent[position] // parts).reshape((-1,) + (1,) * (len(extent) - 1 - position))
    return loudness


def noise(stream_key, shape, scale, most, cuts=(), held_as=jnp.bfloat16):
    result = scale * jax.random.normal(stream_key, shape, jnp.float32)
    if cuts:
        result = result * levels(stream_key, shape, cuts, -0.22, 0.18)
    return jnp.clip(result, -most, most).astype(held_as)


def setup_inputs(seed: int = 0, part: int = 0) -> dict:
    key_list = jax.random.split(jax.random.key(seed), 9)
    part_keys = jax.random.split(jax.random.fold_in(key_list[8], part), 9)
    return {
        "wavefields": noise(part_keys[0], (SHOTS, 2, 9, NZ, NX, NY), 1.0, 6.0, ((0, 4), (3, 32)), jnp.float32),
        "earth_model": jnp.clip(jnp.exp(math.log(1.6) - 1.3862944 * jax.random.uniform(part_keys[1], (3, NZ, NX, NY), jnp.float32) ** levels(part_keys[1], (3, NZ, NX, NY), ((1, 32),), -0.2, 0.2)), 0.4, 1.6),
        "source_depth": plant(jax.random.randint(part_keys[2], (SHOTS,), 0, NZ), jax.random.fold_in(part_keys[2], 1), 0, NZ - 1).astype(jnp.int32),
        "source_column": plant(jax.random.randint(part_keys[3], (SHOTS,), 0, NX * NY), jax.random.fold_in(part_keys[3], 1), 0, (NX * NY) - 1).astype(jnp.int32),
        "wavelet": noise(part_keys[4], (SHOTS, STEPS), 5.0, 30.0, ((0, 4),), jnp.float32),
        "receiver_depth": plant(jax.random.randint(part_keys[5], (SHOTS, RECV), 0, NZ), jax.random.fold_in(part_keys[5], 1), 0, NZ - 1).astype(jnp.int32),
        "receiver_column": plant(jax.random.randint(part_keys[6], (SHOTS, RECV), 0, NX * NY), jax.random.fold_in(part_keys[6], 1), 0, (NX * NY) - 1).astype(jnp.int32),
        "traces": noise(part_keys[7], (SHOTS, STEPS, RECV), 5.0, 30.0, ((0, 4),), jnp.float32),
    }


time_step = 0.15


def forward_diff(array, dim_index):
    length = array.shape[dim_index]
    following = jnp.concatenate([lax.slice_in_dim(array, 1, length, axis=dim_index), jnp.zeros_like(lax.slice_in_dim(array, 0, 1, axis=dim_index))], axis=dim_index)
    return following - array


def backward_diff(array, dim_index):
    length = array.shape[dim_index]
    previous = jnp.concatenate([jnp.zeros_like(lax.slice_in_dim(array, 0, 1, axis=dim_index)), lax.slice_in_dim(array, 0, length - 1, axis=dim_index)], axis=dim_index)
    return array - previous


def depth_forward(array, plane_high):
    following = jnp.concatenate([array[:, 1:], plane_high[:, None]], axis=1)
    return following - array


def depth_backward(array, plane_low):
    previous = jnp.concatenate([plane_low[:, None], array[:, :-1]], axis=1)
    return array - previous


def velocity_half(fields, buoyancy, sxz_low, syz_low, szz_high):
    vel_x, vel_y, vel_z, sig_xx, sig_yy, sig_zz, sig_xy, sig_xz, sig_yz = fields
    vel_x = vel_x + time_step * buoyancy * (forward_diff(sig_xx, 2) + backward_diff(sig_xy, 3) + depth_backward(sig_xz, sxz_low))
    vel_y = vel_y + time_step * buoyancy * (backward_diff(sig_xy, 2) + forward_diff(sig_yy, 3) + depth_backward(sig_yz, syz_low))
    vel_z = vel_z + time_step * buoyancy * (backward_diff(sig_xz, 2) + backward_diff(sig_yz, 3) + depth_forward(sig_zz, szz_high))
    return vel_x, vel_y, vel_z


def stress_half(fields, lame_lambda, shear_mu, vz_low, vx_high, vy_high):
    vel_x, vel_y, vel_z, sig_xx, sig_yy, sig_zz, sig_xy, sig_xz, sig_yz = fields
    strain_x = backward_diff(vel_x, 2)
    strain_y = backward_diff(vel_y, 3)
    strain_z = depth_backward(vel_z, vz_low)
    spread = strain_x + strain_y + strain_z
    sig_xx = sig_xx + time_step * (lame_lambda * spread + 2.0 * shear_mu * strain_x)
    sig_yy = sig_yy + time_step * (lame_lambda * spread + 2.0 * shear_mu * strain_y)
    sig_zz = sig_zz + time_step * (lame_lambda * spread + 2.0 * shear_mu * strain_z)
    vx_up = depth_forward(vel_x, vx_high)
    vy_up = depth_forward(vel_y, vy_high)
    vz_along_x = forward_diff(vel_z, 2)
    vz_along_y = forward_diff(vel_z, 3)
    vx_along_y = forward_diff(vel_x, 3)
    vy_along_x = forward_diff(vel_y, 2)
    sig_xy = sig_xy + time_step * shear_mu * (vx_along_y + vy_along_x)
    sig_xz = sig_xz + time_step * shear_mu * (vx_up + vz_along_x)
    sig_yz = sig_yz + time_step * shear_mu * (vy_up + vz_along_y)
    rotation = (vz_along_y - vy_up) + (vx_up - vz_along_x) + (vy_along_x - vx_along_y)
    return [vel_x, vel_y, vel_z, sig_xx, sig_yy, sig_zz, sig_xy, sig_xz, sig_yz], rotation


def reference(wavefields, earth_model, source_depth, source_column, wavelet, receiver_depth, receiver_column, traces):
    buoyancy = earth_model[0]
    lame_lambda = earth_model[1]
    shear_mu = earth_model[2]
    image_pp = jnp.zeros((NZ, NX, NY), jnp.float32)
    image_ps = jnp.zeros((NZ, NX, NY), jnp.float32)
    zero_plane = jnp.zeros((2, NX, NY), jnp.float32)
    for shot_index in range(SHOTS):
        fields = [wavefields[shot_index, :, field_no] for field_no in range(9)]
        src_row = source_column[shot_index] // NY
        src_col = source_column[shot_index] % NY
        rec_row = receiver_column[shot_index] // NY
        rec_col = receiver_column[shot_index] % NY
        for step_index in range(STEPS):
            vel_x, vel_y, vel_z = velocity_half(fields, buoyancy, zero_plane, zero_plane, zero_plane)
            vel_z = vel_z.at[1, receiver_depth[shot_index], rec_row, rec_col].add(time_step * traces[shot_index, step_index])
            fields, rotation = stress_half([vel_x, vel_y, vel_z] + list(fields[3:]), lame_lambda, shear_mu, zero_plane, zero_plane, zero_plane)
            for field_no in (3, 4, 5):
                fields[field_no] = fields[field_no].at[0, source_depth[shot_index], src_row, src_col].add(time_step * wavelet[shot_index, step_index])
            pressure = (fields[3] + fields[4] + fields[5]) / 3.0
            image_pp = image_pp + pressure[0] * pressure[1]
            image_ps = image_ps + pressure[0] * rotation[1]
    return jnp.stack([image_pp, image_ps]) / STEPS
```

```python
import functools

import jax
import jax.numpy as jnp
from jax import lax
from jax.experimental import pallas as pl
from jax.experimental.pallas import tpu as pltpu
from jax.sharding import PartitionSpec as P


time_step = 0.15
VX, VY, VZ, XX, YY, ZZ, XY, XZ, YZ = range(9)
PAD = 3
TOP = 8


def cyclic(value, axis, steps):
    count = lax.axis_size(axis)
    return lax.ppermute(value, axis, [(s, (s + steps) % count) for s in range(count)])


class Fields:
    def __init__(self, ref, wave, rows):
        self.ref, self.wave, self.rows = ref, wave, rows

    def at(self, field, plane, move=0):
        return self.ref[self.wave, field, plane + PAD, TOP + move : TOP + move + self.rows, :]

    def put(self, field, plane, value):
        self.ref[self.wave, field, plane + PAD, TOP : TOP + self.rows, :] = value


def clear(ref, rows, slab, beyond):
    for wave in range(2):
        for field in range(9):
            for plane in range(slab + 2 * PAD):
                inside = PAD <= plane < PAD + slab
                if not (inside or beyond):
                    continue
                zero = jnp.zeros((8, ref.shape[-1]), jnp.float32)
                ref[wave, field, plane, 0:TOP, :] = zero
                ref[wave, field, plane, TOP + rows : TOP + rows + 8, :] = zero
                if not inside:
                    ref[wave, field, plane, TOP : TOP + rows, :] = jnp.zeros(
                        (rows, ref.shape[-1]), jnp.float32
                    )


def y_next(value):
    count = value.shape[1]
    lane = lax.broadcasted_iota(jnp.int32, value.shape, 1)
    return jnp.where(lane == count - 1, 0.0, pltpu.roll(value, count - 1, 1))


def y_last(value):
    lane = lax.broadcasted_iota(jnp.int32, value.shape, 1)
    return jnp.where(lane == 0, 0.0, pltpu.roll(value, 1, 1))


def minus(a, b):
    return a if b is None else a - b


def from_high(b, a):
    return -a if b is None else b - a


def velocity(old, new, plane, scaled, parts, low_xz, low_yz, high_zz, added=None):
    if "x" in parts:
        xx, xy, xz = old.at(XX, plane), old.at(XY, plane), old.at(XZ, plane)
        change = (old.at(XX, plane, 1) - xx) + (xy - y_last(xy)) + minus(xz, low_xz)
        new.put(VX, plane, old.at(VX, plane) + scaled * change)
    if "y" in parts:
        xy, yy, yz = old.at(XY, plane), old.at(YY, plane), old.at(YZ, plane)
        change = (xy - old.at(XY, plane, -1)) + (y_next(yy) - yy) + minus(yz, low_yz)
        new.put(VY, plane, old.at(VY, plane) + scaled * change)
    if "z" in parts:
        xz, yz, zz = old.at(XZ, plane), old.at(YZ, plane), old.at(ZZ, plane)
        change = (xz - old.at(XZ, plane, -1)) + (yz - y_last(yz)) + from_high(high_zz, zz)
        result = old.at(VZ, plane) + scaled * change
        new.put(VZ, plane, result if added is None else result + added)


def stress(old, new, plane, lam, mu, low_vz, high_vx, high_vy, added=None, turn=False):
    vx, vy, vz = new.at(VX, plane), new.at(VY, plane), new.at(VZ, plane)
    e_x = vx - new.at(VX, plane, -1)
    e_y = vy - y_last(vy)
    e_z = minus(vz, low_vz)
    shared = lam * (e_x + e_y + e_z)
    if added is not None:
        shared = shared + added
    twice = 2.0 * mu
    xx = old.at(XX, plane) + (shared + twice * e_x)
    yy = old.at(YY, plane) + (shared + twice * e_y)
    zz = old.at(ZZ, plane) + (shared + twice * e_z)
    new.put(XX, plane, xx)
    new.put(YY, plane, yy)
    new.put(ZZ, plane, zz)
    vx_up, vy_up = from_high(high_vx, vx), from_high(high_vy, vy)
    vz_x, vy_x = new.at(VZ, plane, 1) - vz, new.at(VY, plane, 1) - vy
    vz_y, vx_y = y_next(vz) - vz, y_next(vx) - vx
    new.put(XY, plane, old.at(XY, plane) + mu * (vx_y + vy_x))
    new.put(XZ, plane, old.at(XZ, plane) + mu * (vx_up + vz_x))
    new.put(YZ, plane, old.at(YZ, plane) + mu * (vy_up + vz_y))
    total = xx + yy + zz
    if not turn:
        return total, None
    return total, (vz_y - vy_up) + (vx_up - vz_x) + (vy_x - vx_y)


def run_alone(first, held, earth, inject, spot, amount, above, below, rows, slab, span, start):
    for level in range(span):
        left = span - 1 - level
        for wave in range(2):
            old = Fields(first if level == 0 else held, wave, rows)
            new = Fields(held, wave, rows)
            for name, field in enumerate((XZ, YZ)):
                above[level, name, wave] = old.at(field, slab - 1)
            below[level, 0, wave] = old.at(ZZ, 0)
            for plane in range(slab):
                near_low, near_high = plane - left, slab - 1 - plane - left
                parts = "".join(
                    part
                    for part in "xyz"
                    if near_low <= (0 if part != "z" else -1)
                    or near_high <= (0 if part == "z" else -1)
                    or left == span - 1
                )
                velocity(
                    old,
                    new,
                    plane,
                    time_step * earth[0, plane],
                    parts if left < 2 else "xyz",
                    old.at(XZ, plane - 1) if plane else None,
                    old.at(YZ, plane - 1) if plane else None,
                    old.at(ZZ, plane + 1) if plane < slab - 1 else None,
                    inject[start + level, plane] if wave == 1 else None,
                )
            above[level, 2, wave] = new.at(VZ, slab - 1)
            below[level, 1, wave] = new.at(VX, 0)
            below[level, 2, wave] = new.at(VY, 0)
            if left == 0:
                continue
            for plane in range(slab):
                if left == 1 and 0 < plane < slab - 1:
                    continue
                stress(
                    old,
                    new,
                    plane,
                    time_step * earth[1, plane],
                    time_step * earth[2, plane],
                    new.at(VZ, plane - 1) if plane else None,
                    new.at(VX, plane + 1) if plane < slab - 1 else None,
                    new.at(VY, plane + 1) if plane < slab - 1 else None,
                    spot[...] * amount(level, plane) if wave == 0 else None,
                )


def run_true(held, earth, low_earth, high_earth, inject, spot, amount, low, high, image,
             keep_low, keep_high, rows, slab, span, start):
    def from_below(level, name, wave):
        return jnp.where(keep_low, low[level, name, wave], 0.0)

    def from_above(level, name, wave):
        return jnp.where(keep_high, high[level, name, wave], 0.0)

    def medium(kind, plane):
        if plane < 0:
            value = jnp.where(keep_low, low_earth[kind, plane + low_earth.shape[1]], 0.0)
        elif plane >= slab:
            value = jnp.where(keep_high, high_earth[kind, plane - slab], 0.0)
        else:
            value = earth[kind, plane]
        return time_step * value

    for level in range(span):
        done, left = level + 1, span - 1 - level
        moving = {}
        for plane in range(slab):
            moving[plane] = "xyz"
        for far in range(1, PAD):
            if done >= far and left >= far - 1:
                first, last = done == far, left == far - 1
                moving[-far] = "z" if first or last else "xyz"
                moving[slab - 1 + far] = "xy" if first or last else "xyz"
        for wave in range(2):
            both = Fields(held, wave, rows)
            for plane, parts in sorted(moving.items()):
                low_xz, low_yz = both.at(XZ, plane - 1), both.at(YZ, plane - 1)
                high_zz = both.at(ZZ, plane + 1)
                if plane == 0:
                    low_xz = low_xz + from_below(level, 0, wave)
                    low_yz = low_yz + from_below(level, 1, wave)
                if plane == slab - 1:
                    high_zz = high_zz + from_above(level, 0, wave)
                own = 0 <= plane < slab
                velocity(
                    both,
                    both,
                    plane,
                    medium(0, plane),
                    parts,
                    low_xz,
                    low_yz,
                    high_zz,
                    inject[start + level, plane] if own and wave == 1 else None,
                )
        shaking = list(range(slab))
        for far in range(1, PAD):
            if done >= far and left >= far:
                shaking += [-far, slab - 1 + far]
        for plane in sorted(shaking):
            own = 0 <= plane < slab
            found = []
            for wave in range(2):
                both = Fields(held, wave, rows)
                low_vz = both.at(VZ, plane - 1)
                high_vx, high_vy = both.at(VX, plane + 1), both.at(VY, plane + 1)
                if plane == 0:
                    low_vz = low_vz + from_below(level, 2, wave)
                if plane == slab - 1:
                    high_vx = high_vx + from_above(level, 1, wave)
                    high_vy = high_vy + from_above(level, 2, wave)
                found.append(
                    stress(
                        both,
                        both,
                        plane,
                        medium(1, plane),
                        medium(2, plane),
                        low_vz,
                        high_vx,
                        high_vy,
                        spot[...] * amount(level, plane) if own and wave == 0 else None,
                        turn=own and wave == 1,
                    )
                )
            if own:
                (source, _), (receiver, rotation) = found
                image[0, plane] += source * receiver
                image[1, plane] += source * rotation


def set_up(numbers, wavelet, spot, start):
    shape = spot.shape
    row = lax.broadcasted_iota(jnp.int32, shape, 0)
    column = lax.broadcasted_iota(jnp.int32, shape, 1)
    hit = (row == numbers[1]) & (column == numbers[2])
    spot[...] = jnp.where(hit, time_step, 0.0)

    def amount(level, plane):
        return jnp.where(numbers[0] == plane, wavelet[start + level], 0.0)

    return amount


def first_kernel(sizes, wavefields, earth, numbers, wavelet, rows_of, columns_of, traces,
                 above, below, inject, first, held, spot, arrived):
    rows, slab, span, steps = sizes
    fetch = pltpu.make_async_copy(
        wavefields.at[0], first.at[:, :, PAD : PAD + slab, TOP : TOP + rows, :], arrived
    )
    fetch.start()
    width = spot.shape[1]
    receivers = rows_of.shape[1]
    which = lax.broadcasted_iota(jnp.int32, (slab * rows, receivers), 0) == rows_of[...]
    which = which.astype(jnp.float32)
    where = lax.broadcasted_iota(jnp.int32, (receivers, width), 1) == columns_of[...]
    for step in range(steps):
        table = jnp.where(where, time_step * traces[:, step : step + 1], 0.0)
        dense = jnp.dot(
            which, table, precision=lax.Precision.HIGHEST, preferred_element_type=jnp.float32
        )
        inject[step] = dense.reshape(slab, rows, width)
    clear(first, rows, slab, False)
    clear(held, rows, slab, False)
    amount = set_up(numbers, wavelet, spot, 0)
    fetch.wait()
    run_alone(first, held, earth, inject, spot, amount, above, below, rows, slab, span, 0)


def middle_kernel(sizes, wavefields, earth, low_earth, high_earth, numbers, wavelet, inject,
                  low, high, fields, image, above, below, first, held, spot, arrived):
    rows, slab, span, steps = sizes
    inside = first.at[:, :, PAD : PAD + slab, TOP : TOP + rows, :]
    fetch = pltpu.make_async_copy(wavefields.at[0], inside, arrived)
    fetch.start()
    clear(first, rows, slab, True)
    clear(held, rows, slab, False)
    amount = set_up(numbers, wavelet, spot, 0)
    later = set_up(numbers, wavelet, spot, span)
    image[...] = jnp.zeros_like(image)
    fetch.wait()
    run_true(first, earth, low_earth, high_earth, inject, spot, amount, low, high, image,
             numbers[3] > 0, numbers[4] > 0, rows, slab, span, 0)
    store = pltpu.make_async_copy(inside, fields, arrived)
    store.start()
    run_alone(first, held, earth, inject, spot, later, above, below, rows, slab, span, span)
    store.wait()


def last_kernel(sizes, fields, so_far, earth, low_earth, high_earth, numbers, wavelet, inject,
                low, high, image, first, spot, arrived):
    rows, slab, span, steps = sizes
    fetch = pltpu.make_async_copy(
        fields, first.at[:, :, PAD : PAD + slab, TOP : TOP + rows, :], arrived
    )
    fetch.start()
    clear(first, rows, slab, True)
    amount = set_up(numbers, wavelet, spot, span)
    image[...] = so_far[...]
    fetch.wait()
    run_true(first, earth, low_earth, high_earth, inject, spot, amount, low, high, image,
             numbers[3] > 0, numbers[4] > 0, rows, slab, span, span)


def on_device(
    wavefields,
    earth_model,
    source_depth,
    source_column,
    wavelet,
    receiver_depth,
    receiver_column,
    traces,
):
    _, waves, _, slab, rows, width = wavefields.shape
    steps = wavelet.shape[1]
    span = slab
    assert steps == 2 * span
    sizes = (rows, slab, span, steps)
    position = lax.axis_index("gz")
    offset = position * slab
    numbers = jnp.stack(
        [
            source_depth[0] - offset,
            source_column[0] // width,
            source_column[0] % width,
            position,
            lax.axis_size("gz") - 1 - position,
        ]
    ).astype(jnp.int32)
    rows_of = (receiver_depth - offset) * rows + receiver_column // width
    columns_of = (receiver_column % width).reshape(-1, 1)
    by_receiver = traces[0].T

    low_earth = cyclic(earth_model[:, slab - 2 :], "gz", 1)
    high_earth = cyclic(earth_model[:, :2], "gz", -1)

    vmem = pl.BlockSpec(memory_space=pltpu.VMEM)
    smem = pl.BlockSpec(memory_space=pltpu.SMEM)
    anywhere = pl.BlockSpec(memory_space=pl.ANY)
    held = pltpu.VMEM((waves, 9, slab + 2 * PAD, rows + 16, width), jnp.float32)
    spot = pltpu.VMEM((rows, width), jnp.float32)
    arrived = pltpu.SemaphoreType.DMA
    history = jax.ShapeDtypeStruct((span, 3, waves, rows, width), jnp.float32)
    dense = jax.ShapeDtypeStruct((steps, slab, rows, width), jnp.float32)
    images = jax.ShapeDtypeStruct((2, slab, rows, width), jnp.float32)
    kept = jax.ShapeDtypeStruct(wavefields.shape[1:], jnp.float32)
    work = waves * 9 * slab * rows * width

    def cost(scale):
        return pl.CostEstimate(flops=scale * work, bytes_accessed=4 * work, transcendentals=0)

    above, below, inject = pl.pallas_call(
        functools.partial(first_kernel, sizes),
        out_shape=(history, history, dense),
        in_specs=[anywhere, vmem, smem, smem, vmem, vmem, vmem],
        out_specs=(vmem, vmem, vmem),
        scratch_shapes=[held, held, spot, arrived],
        cost_estimate=cost(40),
        name="first",
    )(wavefields, earth_model, numbers, wavelet[0], rows_of, columns_of, by_receiver)
    low = cyclic(above, "gz", 1)
    high = cyclic(below, "gz", -1)
    fields, image, above, below = pl.pallas_call(
        functools.partial(middle_kernel, sizes),
        out_shape=(kept, images, history, history),
        in_specs=[anywhere, vmem, vmem, vmem, smem, smem, vmem, vmem, vmem],
        out_specs=(anywhere, vmem, vmem, vmem),
        scratch_shapes=[held, held, spot, arrived],
        cost_estimate=cost(100),
        name="middle",
    )(wavefields, earth_model, low_earth, high_earth, numbers, wavelet[0], inject, low, high)
    low = cyclic(above, "gz", 1)
    high = cyclic(below, "gz", -1)
    image = pl.pallas_call(
        functools.partial(last_kernel, sizes),
        out_shape=images,
        in_specs=[anywhere, vmem, vmem, vmem, vmem, smem, smem, vmem, vmem, vmem],
        out_specs=vmem,
        scratch_shapes=[held, spot, arrived],
        cost_estimate=cost(60),
        name="last",
    )(fields, image, earth_model, low_earth, high_earth, numbers, wavelet[0], inject, low, high)

    total = image
    for far in range(1, lax.axis_size("shot")):
        total = total + cyclic(image, "shot", far)
    return total * jnp.array([1.0 / (9 * steps), 1.0 / (3 * steps)], jnp.float32).reshape(2, 1, 1, 1)


def solution(mesh):
    placed = (
        P(("parts", "shot"), None, None, "gz", None, None),
        P("parts", "gz", None, None),
        P(("parts", "shot")),
        P(("parts", "shot")),
        P(("parts", "shot"), None),
        P(("parts", "shot"), None),
        P(("parts", "shot"), None),
        P(("parts", "shot"), None, None),
    )
    return jax.shard_map(
        on_device,
        mesh=mesh,
        in_specs=placed,
        out_specs=P("parts", "gz", None, None),
        check_vma=False,
    )
```

```python
import functools

import jax
import jax.numpy as jnp
from jax import lax
from jax.experimental import pallas as pl
from jax.experimental.pallas import tpu as pltpu
from jax.sharding import PartitionSpec as P


time_step = 0.15
VX, VY, VZ, XX, YY, ZZ, XY, XZ, YZ = range(9)
PAD = 3
TOP = 8
LIMIT = 24 * 1024 * 1024


def cyclic(value, axis, steps):
    count = lax.axis_size(axis)
    return lax.ppermute(value, axis, [(s, (s + steps) % count) for s in range(count)])


def swapped(value, axis, first):
    count = lax.axis_size(axis)
    partner = {s: s for s in range(count)}
    for s in range(first, count - 1, 2):
        partner[s], partner[s + 1] = s + 1, s
    return lax.ppermute(value, axis, sorted(partner.items()))


class Fields:
    def __init__(self, ref, wave, rows):
        self.ref, self.wave, self.rows = ref, wave, rows

    def at(self, field, plane, move=0):
        return self.ref[self.wave, field, plane + PAD, TOP + move : TOP + move + self.rows, :]

    def put(self, field, plane, value):
        self.ref[self.wave, field, plane + PAD, TOP : TOP + self.rows, :] = value


def clear_margins(ref, rows, planes):
    zero = jnp.zeros((8, ref.shape[-1]), jnp.float32)
    for wave in range(2):
        for field in range(9):
            for plane in planes:
                ref[wave, field, plane + PAD, 0:TOP, :] = zero
                ref[wave, field, plane + PAD, TOP + rows : TOP + rows + 8, :] = zero


def clear_planes(ref, rows, planes):
    zero = jnp.zeros((rows, ref.shape[-1]), jnp.float32)
    for wave in range(2):
        for field in range(9):
            for plane in planes:
                ref[wave, field, plane + PAD, TOP : TOP + rows, :] = zero


def beyond(slab):
    return [*range(-PAD, 0), *range(slab, slab + PAD)]


def y_next(value):
    count = value.shape[1]
    lane = lax.broadcasted_iota(jnp.int32, value.shape, 1)
    return jnp.where(lane == count - 1, 0.0, pltpu.roll(value, count - 1, 1))


def y_last(value):
    lane = lax.broadcasted_iota(jnp.int32, value.shape, 1)
    return jnp.where(lane == 0, 0.0, pltpu.roll(value, 1, 1))


def minus(a, b):
    return a if b is None else a - b


def from_high(b, a):
    return -a if b is None else b - a


def velocity(old, new, plane, scaled, parts, low_xz, low_yz, high_zz, added=None):
    if "x" in parts:
        xx, xy, xz = old.at(XX, plane), old.at(XY, plane), old.at(XZ, plane)
        change = (old.at(XX, plane, 1) - xx) + (xy - y_last(xy)) + minus(xz, low_xz)
        new.put(VX, plane, old.at(VX, plane) + scaled * change)
    if "y" in parts:
        xy, yy, yz = old.at(XY, plane), old.at(YY, plane), old.at(YZ, plane)
        change = (xy - old.at(XY, plane, -1)) + (y_next(yy) - yy) + minus(yz, low_yz)
        new.put(VY, plane, old.at(VY, plane) + scaled * change)
    if "z" in parts:
        xz, yz, zz = old.at(XZ, plane), old.at(YZ, plane), old.at(ZZ, plane)
        change = (xz - old.at(XZ, plane, -1)) + (yz - y_last(yz)) + from_high(high_zz, zz)
        result = old.at(VZ, plane) + scaled * change
        new.put(VZ, plane, result if added is None else result + added)


def stress(old, new, plane, lam, mu, twice, low_vz, high_vx, high_vy, added=None, turn=False):
    vx, vy, vz = new.at(VX, plane), new.at(VY, plane), new.at(VZ, plane)
    e_x = vx - new.at(VX, plane, -1)
    e_y = vy - y_last(vy)
    e_z = minus(vz, low_vz)
    shared = lam * (e_x + e_y + e_z)
    if added is not None:
        shared = shared + added
    xx = old.at(XX, plane) + (shared + twice * e_x)
    yy = old.at(YY, plane) + (shared + twice * e_y)
    zz = old.at(ZZ, plane) + (shared + twice * e_z)
    new.put(XX, plane, xx)
    new.put(YY, plane, yy)
    new.put(ZZ, plane, zz)
    vx_up, vy_up = from_high(high_vx, vx), from_high(high_vy, vy)
    vz_x, vy_x = new.at(VZ, plane, 1) - vz, new.at(VY, plane, 1) - vy
    vz_y, vx_y = y_next(vz) - vz, y_next(vx) - vx
    new.put(XY, plane, old.at(XY, plane) + mu * (vx_y + vy_x))
    new.put(XZ, plane, old.at(XZ, plane) + mu * (vx_up + vz_x))
    new.put(YZ, plane, old.at(YZ, plane) + mu * (vy_up + vz_y))
    total = xx + yy + zz
    if not turn:
        return total, None
    return total, (vz_y - vy_up) + (vx_up - vz_x) + (vy_x - vx_y)


def slot(level, name, wave):
    return (level * 3 + name) * 2 + wave


def run_alone(first, held, medium, inject, source, even, chip, cross, rows, slab, span, start):
    for level in range(span):
        left = span - 1 - level
        for wave in range(2):
            old = Fields(first if level == 0 else held, wave, rows)
            new = Fields(held, wave, rows)
            for plane in range(slab):
                near_low, near_high = plane - left, slab - 1 - plane - left
                parts = "xyz"
                if left < 2:
                    parts = "".join(
                        part
                        for part in "xyz"
                        if near_low <= (-1 if part == "z" else 0)
                        or near_high <= (0 if part == "z" else -1)
                    )
                velocity(
                    old,
                    new,
                    plane,
                    medium[0, plane],
                    parts,
                    old.at(XZ, plane - 1) if plane else None,
                    old.at(YZ, plane - 1) if plane else None,
                    old.at(ZZ, plane + 1) if plane < slab - 1 else None,
                    inject[start + level, plane] if wave == 1 else None,
                )
            top = slab - 1
            above = (old.at(XZ, top), new.at(VZ, top), old.at(YZ, top))
            below = (old.at(ZZ, 0), new.at(VX, 0), new.at(VY, 0))
            for name in range(3):
                chip[slot(level, name, wave)] = jnp.where(even, above[name], below[name])
                cross[slot(level, name, wave)] = jnp.where(even, below[name], above[name])
            if left == 0:
                continue
            for plane in range(slab):
                if left == 1 and 0 < plane < slab - 1:
                    continue
                stress(
                    old,
                    new,
                    plane,
                    medium[1, plane],
                    medium[2, plane],
                    medium[3, plane],
                    new.at(VZ, plane - 1) if plane else None,
                    new.at(VX, plane + 1) if plane < slab - 1 else None,
                    new.at(VY, plane + 1) if plane < slab - 1 else None,
                    source[start + level, plane] if wave == 0 else None,
                )


def run_true(held, medium, halo, inject, source, flags, chip, cross, image, fresh,
             rows, slab, span, start):
    even, keep_low, keep_high = flags

    def from_below(level, name, wave):
        at = slot(level, name, wave)
        return jnp.where(keep_low, jnp.where(even, cross[at], chip[at]), 0.0)

    def from_above(level, name, wave):
        at = slot(level, name, wave)
        return jnp.where(keep_high, jnp.where(even, chip[at], cross[at]), 0.0)

    def around(kind, plane):
        if plane < 0:
            return halo[0, kind, plane + 2]
        if plane >= slab:
            return halo[1, kind, plane - slab]
        return medium[kind, plane]

    for level in range(span):
        done, left = level + 1, span - 1 - level
        moving = {plane: "xyz" for plane in range(slab)}
        for far in range(1, PAD):
            if done >= far and left >= far - 1:
                edge = done == far or left == far - 1
                moving[-far] = "z" if edge else "xyz"
                moving[slab - 1 + far] = "xy" if edge else "xyz"
        for wave in range(2):
            both = Fields(held, wave, rows)
            for plane, parts in sorted(moving.items()):
                low_xz, low_yz = both.at(XZ, plane - 1), both.at(YZ, plane - 1)
                high_zz = both.at(ZZ, plane + 1)
                if plane == 0:
                    low_xz = low_xz + from_below(level, 0, wave)
                    low_yz = low_yz + from_below(level, 2, wave)
                if plane == slab - 1:
                    high_zz = high_zz + from_above(level, 0, wave)
                own = 0 <= plane < slab
                velocity(
                    both,
                    both,
                    plane,
                    around(0, plane),
                    parts,
                    low_xz,
                    low_yz,
                    high_zz,
                    inject[start + level, plane] if own and wave == 1 else None,
                )
        shaking = list(range(slab))
        for far in range(1, PAD):
            if done >= far and left >= far:
                shaking += [-far, slab - 1 + far]
        for plane in sorted(shaking):
            own = 0 <= plane < slab
            found = []
            for wave in range(2):
                both = Fields(held, wave, rows)
                low_vz = both.at(VZ, plane - 1)
                high_vx, high_vy = both.at(VX, plane + 1), both.at(VY, plane + 1)
                if plane == 0:
                    low_vz = low_vz + from_below(level, 1, wave)
                if plane == slab - 1:
                    high_vx = high_vx + from_above(level, 1, wave)
                    high_vy = high_vy + from_above(level, 2, wave)
                found.append(
                    stress(
                        both,
                        both,
                        plane,
                        around(1, plane),
                        around(2, plane),
                        around(3, plane),
                        low_vz,
                        high_vx,
                        high_vy,
                        source[start + level, plane] if own and wave == 0 else None,
                        turn=own and wave == 1,
                    )
                )
            if own:
                (given, _), (taken, rotation) = found
                if fresh and level == 0:
                    image[0, plane] = given * taken
                    image[1, plane] = given * rotation
                else:
                    image[0, plane] += given * taken
                    image[1, plane] += given * rotation


def where_am_i():
    position = lax.axis_index("gz")
    return position % 2 == 0, position > 0, position < lax.axis_size("gz") - 1


def dense_points(depth, column, amounts, slab, rows, width, offset, steps, put):
    points = depth.shape[1]
    row = (depth - offset) * rows + column // width
    where = lax.broadcasted_iota(jnp.int32, (width, points), 0) == column % width
    where = where.astype(jnp.bfloat16)
    where = jnp.concatenate([where, where, where], axis=1)
    which = lax.broadcasted_iota(jnp.int32, (slab * rows, points), 0) == row
    for step in range(steps):
        whole = jnp.where(which, time_step * amounts[step : step + 1, :], 0.0)
        high = whole.astype(jnp.bfloat16)
        rest = whole - high.astype(jnp.float32)
        middle = rest.astype(jnp.bfloat16)
        low = (rest - middle.astype(jnp.float32)).astype(jnp.bfloat16)
        planes = lax.dot_general(
            jnp.concatenate([high, middle, low], axis=1),
            where,
            (((1,), (1,)), ((), ())),
            preferred_element_type=jnp.float32,
        )
        put(step, planes.reshape(slab, rows, width))


def first_kernel(sizes, wavefields, earth, *refs):
    rows, width, slab, span, steps = sizes
    scalars, outside, results, inside = refs[:2], refs[2:6], refs[6:12], refs[12:16]
    held, arrived = refs[16:]
    chip, cross, fields, medium, inject, source = results
    source_depth, source_column = scalars
    wavelet, depth, column, traces = inside
    pairs = [*zip(outside, inside), (earth, medium.at[0:3])]
    pairs.append((wavefields.at[0], fields.at[:, :, PAD : PAD + slab, TOP : TOP + rows, :]))
    fetches = [pltpu.make_async_copy(*pair, arrived.at[n]) for n, pair in enumerate(pairs)]
    for fetch in fetches:
        fetch.start()
    clear_margins(fields, rows, range(-PAD, slab + PAD))
    clear_planes(fields, rows, beyond(slab))
    clear_margins(held, rows, range(slab))
    for fetch in fetches[:4]:
        fetch.wait()
    position = lax.axis_index("gz")
    even = position % 2 == 0

    def put(step, planes):
        inject[step] = planes

    dense_points(depth[...], column[...], traces[0], slab, rows, width, position * slab, steps, put)
    row = lax.broadcasted_iota(jnp.int32, (rows, width), 0)
    lane = lax.broadcasted_iota(jnp.int32, (rows, width), 1)
    spot = row * width + lane == source_column[0]
    for plane in range(slab):
        here = source_depth[0] == position * slab + plane
        for step in range(steps):
            amount = jnp.where(here, time_step * wavelet[0, step], 0.0)
            source[step, plane] = jnp.where(spot, amount, 0.0)
    fetches[4].wait()
    for kind in range(3):
        medium[kind] = time_step * medium[kind]
    medium[3] = 2.0 * medium[2]
    for kind in range(3):
        for far in range(2):
            at = slot(span, 0, 0) + kind * 2 + far
            above, below = medium[kind, slab - 2 + far], medium[kind, far]
            chip[at] = jnp.where(even, above, below)
            cross[at] = jnp.where(even, below, above)
    fetches[5].wait()
    run_alone(fields, held, medium, inject, source, even, chip, cross, rows, slab, span, 0)


def middle_kernel(sizes, fields_in, medium, inject, source, chip, cross,
                  fields, halo, image, next_chip, next_cross, held):
    rows, width, slab, span, steps = sizes
    flags = even, keep_low, keep_high = where_am_i()
    for kind in range(3):
        for far in range(2):
            at = slot(span, 0, 0) + kind * 2 + far
            low = jnp.where(keep_low, jnp.where(even, cross[at], chip[at]), 0.0)
            high = jnp.where(keep_high, jnp.where(even, chip[at], cross[at]), 0.0)
            halo[0, kind, far] = low
            halo[1, kind, far] = high
            if kind == 2:
                halo[0, 3, far] = 2.0 * low
                halo[1, 3, far] = 2.0 * high
    clear_margins(held, rows, range(slab))
    run_true(fields, medium, halo, inject, source, flags, chip, cross, image, True,
             rows, slab, span, 0)
    run_alone(fields, held, medium, inject, source, even, next_chip, next_cross,
              rows, slab, span, span)
    clear_planes(fields, rows, beyond(slab))


def last_kernel(sizes, fields_in, medium, halo, inject, source, chip, cross, so_far,
                fields, image):
    rows, width, slab, span, steps = sizes
    image[...] = so_far[...]
    run_true(fields, medium, halo, inject, source, where_am_i(), chip, cross, image, False,
             rows, slab, span, span)


def within(space, *arrays):
    return [pltpu.with_memory_space_constraint(a, space) for a in arrays]


def on_device(
    wavefields,
    earth_model,
    source_depth,
    source_column,
    wavelet,
    receiver_depth,
    receiver_column,
    traces,
):
    _, waves, _, slab, rows, width = wavefields.shape
    steps = wavelet.shape[1]
    span = slab
    assert steps == 2 * span
    sizes = (rows, width, slab, span, steps)

    vmem = pl.BlockSpec(memory_space=pltpu.VMEM)
    smem = pl.BlockSpec(memory_space=pltpu.SMEM)
    anywhere = pl.BlockSpec(memory_space=pl.ANY)

    def room(*shape):
        return pltpu.VMEM(shape, jnp.float32)

    state = room(waves, 9, slab + 2 * PAD, rows + 16, width)
    history = room(slot(span, 0, 0), rows, width)
    with_medium = room(slot(span, 0, 0) + 6, rows, width)
    dense = room(steps, slab, rows, width)
    images = room(2, slab, rows, width)
    work = waves * 9 * slab * rows * width

    def options(scale):
        return dict(
            cost_estimate=pl.CostEstimate(
                flops=scale * work, bytes_accessed=4 * work, transcendentals=0
            ),
            compiler_params=pltpu.CompilerParams(vmem_limit_bytes=LIMIT),
        )

    chip, cross, fields, medium, inject, source = pl.pallas_call(
        functools.partial(first_kernel, sizes),
        out_shape=(with_medium, with_medium, state, room(4, slab, rows, width), dense, dense),
        in_specs=[anywhere, anywhere, smem, smem] + [anywhere] * 4,
        out_specs=(vmem,) * 6,
        scratch_shapes=[
            pltpu.SMEM(wavelet.shape, jnp.float32),
            pltpu.VMEM(receiver_depth.shape, jnp.int32),
            pltpu.VMEM(receiver_column.shape, jnp.int32),
            room(*traces.shape),
            state,
            pltpu.SemaphoreType.DMA((6,)),
        ],
        name="first",
        **options(40),
    )(*within(pltpu.HBM, wavefields, earth_model), source_depth, source_column,
      *within(pltpu.HBM, wavelet, receiver_depth, receiver_column, traces))
    cross = swapped(cross, "gz", 1)
    chip = swapped(chip, "gz", 0)
    fields, halo, image, chip, cross = pl.pallas_call(
        functools.partial(middle_kernel, sizes),
        out_shape=(state, room(2, 4, 2, rows, width), images, history, history),
        in_specs=[vmem] * 6,
        out_specs=(vmem,) * 5,
        scratch_shapes=[state],
        input_output_aliases={0: 0},
        name="middle",
        **options(100),
    )(*within(pltpu.VMEM, fields, medium, inject, source, chip, cross))
    cross = swapped(cross, "gz", 1)
    chip = swapped(chip, "gz", 0)
    _, image = pl.pallas_call(
        functools.partial(last_kernel, sizes),
        out_shape=(state, images),
        in_specs=[vmem] * 8,
        out_specs=(vmem,) * 2,
        input_output_aliases={0: 0},
        name="last",
        **options(60),
    )(*within(pltpu.VMEM, fields, medium, halo, inject, source, chip, cross, image))

    total = image
    for far in range(1, lax.axis_size("shot")):
        total = total + cyclic(image, "shot", far)
    kind = lax.broadcasted_iota(jnp.int32, total.shape, 0)
    return total * jnp.where(kind == 0, 1.0 / (9 * steps), 1.0 / (3 * steps))


def solution(mesh):
    placed = (
        P(("parts", "shot"), None, None, "gz", None, None),
        P("parts", "gz", None, None),
        P(("parts", "shot")),
        P(("parts", "shot")),
        P(("parts", "shot"), None),
        P(("parts", "shot"), None),
        P(("parts", "shot"), None),
        P(("parts", "shot"), None, None),
    )
    return jax.shard_map(
        on_device,
        mesh=mesh,
        in_specs=placed,
        out_specs=P("parts", "gz", None, None),
        check_vma=False,
    )
```

```python
import functools

import jax
import jax.numpy as jnp
from jax import lax
from jax.experimental import pallas as pl
from jax.experimental.pallas import tpu as pltpu
from jax.sharding import PartitionSpec as P


time_step = 0.15
VX, VY, VZ, XX, YY, ZZ, XY, XZ, YZ = range(9)
PAD = 3
TOP = 8
LIMIT = 24 * 1024 * 1024


def cyclic(value, axis, steps):
    count = lax.axis_size(axis)
    return lax.ppermute(value, axis, [(s, (s + steps) % count) for s in range(count)])


def swapped(value, axis, first):
    count = lax.axis_size(axis)
    partner = {s: s for s in range(count)}
    for s in range(first, count - 1, 2):
        partner[s], partner[s + 1] = s + 1, s
    return lax.ppermute(value, axis, sorted(partner.items()))


class Fields:
    def __init__(self, ref, wave, rows):
        self.ref, self.wave, self.rows = ref, wave, rows

    def at(self, field, plane, move=0):
        return self.ref[self.wave, field, plane + PAD, TOP + move : TOP + move + self.rows, :]

    def put(self, field, plane, value):
        self.ref[self.wave, field, plane + PAD, TOP : TOP + self.rows, :] = value


def clear_margins(ref, rows, planes):
    zero = jnp.zeros((8, ref.shape[-1]), jnp.float32)
    for wave in range(2):
        for field in range(9):
            for plane in planes:
                ref[wave, field, plane + PAD, 0:TOP, :] = zero
                ref[wave, field, plane + PAD, TOP + rows : TOP + rows + 8, :] = zero


def clear_planes(ref, rows, planes):
    zero = jnp.zeros((rows, ref.shape[-1]), jnp.float32)
    for wave in range(2):
        for field in range(9):
            for plane in planes:
                ref[wave, field, plane + PAD, TOP : TOP + rows, :] = zero


def beyond(slab):
    return [*range(-PAD, 0), *range(slab, slab + PAD)]


def y_next(value):
    count = value.shape[1]
    lane = lax.broadcasted_iota(jnp.int32, value.shape, 1)
    return jnp.where(lane == count - 1, 0.0, pltpu.roll(value, count - 1, 1))


def y_last(value):
    lane = lax.broadcasted_iota(jnp.int32, value.shape, 1)
    return jnp.where(lane == 0, 0.0, pltpu.roll(value, 1, 1))


def minus(a, b):
    return a if b is None else a - b


def from_high(b, a):
    return -a if b is None else b - a


def velocity(old, new, plane, scaled, parts, low_xz, low_yz, high_zz, added=None):
    if "x" in parts:
        xx, xy, xz = old.at(XX, plane), old.at(XY, plane), old.at(XZ, plane)
        change = (old.at(XX, plane, 1) - xx) + (xy - y_last(xy)) + minus(xz, low_xz)
        new.put(VX, plane, old.at(VX, plane) + scaled * change)
    if "y" in parts:
        xy, yy, yz = old.at(XY, plane), old.at(YY, plane), old.at(YZ, plane)
        change = (xy - old.at(XY, plane, -1)) + (y_next(yy) - yy) + minus(yz, low_yz)
        new.put(VY, plane, old.at(VY, plane) + scaled * change)
    if "z" in parts:
        xz, yz, zz = old.at(XZ, plane), old.at(YZ, plane), old.at(ZZ, plane)
        change = (xz - old.at(XZ, plane, -1)) + (yz - y_last(yz)) + from_high(high_zz, zz)
        result = old.at(VZ, plane) + scaled * change
        new.put(VZ, plane, result if added is None else result + added)


def stress(old, new, plane, lam, mu, twice, low_vz, high_vx, high_vy, added=None, turn=False):
    vx, vy, vz = new.at(VX, plane), new.at(VY, plane), new.at(VZ, plane)
    e_x = vx - new.at(VX, plane, -1)
    e_y = vy - y_last(vy)
    e_z = minus(vz, low_vz)
    shared = lam * (e_x + e_y + e_z)
    if added is not None:
        shared = shared + added
    xx = old.at(XX, plane) + (shared + twice * e_x)
    yy = old.at(YY, plane) + (shared + twice * e_y)
    zz = old.at(ZZ, plane) + (shared + twice * e_z)
    new.put(XX, plane, xx)
    new.put(YY, plane, yy)
    new.put(ZZ, plane, zz)
    vx_up, vy_up = from_high(high_vx, vx), from_high(high_vy, vy)
    vz_x, vy_x = new.at(VZ, plane, 1) - vz, new.at(VY, plane, 1) - vy
    vz_y, vx_y = y_next(vz) - vz, y_next(vx) - vx
    new.put(XY, plane, old.at(XY, plane) + mu * (vx_y + vy_x))
    new.put(XZ, plane, old.at(XZ, plane) + mu * (vx_up + vz_x))
    new.put(YZ, plane, old.at(YZ, plane) + mu * (vy_up + vz_y))
    total = xx + yy + zz
    if not turn:
        return total, None
    return total, (vz_y - vy_up) + (vx_up - vz_x) + (vy_x - vx_y)


def slot(level, name, wave):
    return (level * 3 + name) * 2 + wave


def run_alone(first, held, medium, inject, source, even, chip, cross, rows, slab, span, start):
    for level in range(span):
        left = span - 1 - level
        for wave in range(2):
            old = Fields(first if level == 0 else held, wave, rows)
            new = Fields(held, wave, rows)
            for plane in range(slab):
                near_low, near_high = plane - left, slab - 1 - plane - left
                parts = "xyz"
                if left < 2:
                    parts = "".join(
                        part
                        for part in "xyz"
                        if near_low <= (-1 if part == "z" else 0)
                        or near_high <= (0 if part == "z" else -1)
                    )
                velocity(
                    old,
                    new,
                    plane,
                    medium[0, plane],
                    parts,
                    old.at(XZ, plane - 1) if plane else None,
                    old.at(YZ, plane - 1) if plane else None,
                    old.at(ZZ, plane + 1) if plane < slab - 1 else None,
                    inject[start + level, plane] if wave == 1 else None,
                )
            top = slab - 1
            above = (old.at(XZ, top), new.at(VZ, top), old.at(YZ, top))
            below = (old.at(ZZ, 0), new.at(VX, 0), new.at(VY, 0))
            for name in range(3):
                chip[slot(level, name, wave)] = jnp.where(even, above[name], below[name])
                cross[slot(level, name, wave)] = jnp.where(even, below[name], above[name])
            if left == 0:
                continue
            for plane in range(slab):
                if left == 1 and 0 < plane < slab - 1:
                    continue
                stress(
                    old,
                    new,
                    plane,
                    medium[1, plane],
                    medium[2, plane],
                    medium[3, plane],
                    new.at(VZ, plane - 1) if plane else None,
                    new.at(VX, plane + 1) if plane < slab - 1 else None,
                    new.at(VY, plane + 1) if plane < slab - 1 else None,
                    source[start + level, plane] if wave == 0 else None,
                )


def run_true(held, medium, halo, inject, source, flags, chip, cross, image, fresh,
             rows, slab, span, start):
    even, keep_low, keep_high = flags

    def from_below(level, name, wave):
        at = slot(level, name, wave)
        return jnp.where(keep_low, jnp.where(even, cross[at], chip[at]), 0.0)

    def from_above(level, name, wave):
        at = slot(level, name, wave)
        return jnp.where(keep_high, jnp.where(even, chip[at], cross[at]), 0.0)

    def around(kind, plane):
        if plane < 0:
            return halo[0, kind, plane + 2]
        if plane >= slab:
            return halo[1, kind, plane - slab]
        return medium[kind, plane]

    for level in range(span):
        done, left = level + 1, span - 1 - level
        moving = {plane: "xyz" for plane in range(slab)}
        for far in range(1, PAD):
            if done >= far and left >= far - 1:
                edge = done == far or left == far - 1
                moving[-far] = "z" if edge else "xyz"
                moving[slab - 1 + far] = "xy" if edge else "xyz"
        for wave in range(2):
            both = Fields(held, wave, rows)
            for plane, parts in sorted(moving.items()):
                low_xz, low_yz = both.at(XZ, plane - 1), both.at(YZ, plane - 1)
                high_zz = both.at(ZZ, plane + 1)
                if plane == 0:
                    low_xz = low_xz + from_below(level, 0, wave)
                    low_yz = low_yz + from_below(level, 2, wave)
                if plane == slab - 1:
                    high_zz = high_zz + from_above(level, 0, wave)
                own = 0 <= plane < slab
                velocity(
                    both,
                    both,
                    plane,
                    around(0, plane),
                    parts,
                    low_xz,
                    low_yz,
                    high_zz,
                    inject[start + level, plane] if own and wave == 1 else None,
                )
        shaking = list(range(slab))
        for far in range(1, PAD):
            if done >= far and left >= far:
                shaking += [-far, slab - 1 + far]
        for plane in sorted(shaking):
            own = 0 <= plane < slab
            found = []
            for wave in range(2):
                both = Fields(held, wave, rows)
                low_vz = both.at(VZ, plane - 1)
                high_vx, high_vy = both.at(VX, plane + 1), both.at(VY, plane + 1)
                if plane == 0:
                    low_vz = low_vz + from_below(level, 1, wave)
                if plane == slab - 1:
                    high_vx = high_vx + from_above(level, 1, wave)
                    high_vy = high_vy + from_above(level, 2, wave)
                found.append(
                    stress(
                        both,
                        both,
                        plane,
                        around(1, plane),
                        around(2, plane),
                        around(3, plane),
                        low_vz,
                        high_vx,
                        high_vy,
                        source[start + level, plane] if own and wave == 0 else None,
                        turn=own and wave == 1,
                    )
                )
            if own:
                (given, _), (taken, rotation) = found
                if fresh and level == 0:
                    image[0, plane] = given * taken
                    image[1, plane] = given * rotation
                else:
                    image[0, plane] += given * taken
                    image[1, plane] += given * rotation


def where_am_i():
    position = lax.axis_index("gz")
    return position % 2 == 0, position > 0, position < lax.axis_size("gz") - 1


def dense_points(depth, column, amounts, slab, rows, width, offset, steps, put):
    points = depth.shape[1]
    row = (depth - offset) * rows + column // width
    where = lax.broadcasted_iota(jnp.int32, (width, points), 0) == column % width
    where = where.astype(jnp.bfloat16)
    where = jnp.concatenate([where, where, where], axis=1)
    which = lax.broadcasted_iota(jnp.int32, (slab * rows, points), 0) == row
    for step in range(steps):
        whole = jnp.where(which, time_step * amounts[step : step + 1, :], 0.0)
        high = whole.astype(jnp.bfloat16)
        rest = whole - high.astype(jnp.float32)
        middle = rest.astype(jnp.bfloat16)
        low = (rest - middle.astype(jnp.float32)).astype(jnp.bfloat16)
        planes = lax.dot_general(
            jnp.concatenate([high, middle, low], axis=1),
            where,
            (((1,), (1,)), ((), ())),
            preferred_element_type=jnp.float32,
        )
        put(step, planes.reshape(slab, rows, width))


def first_kernel(sizes, wavefields, earth, *refs):
    rows, width, slab, span, steps = sizes
    scalars, outside, results, inside = refs[:2], refs[2:6], refs[6:12], refs[12:16]
    held, arrived = refs[16:]
    chip, cross, fields, medium, inject, source = results
    source_depth, source_column = scalars
    wavelet, depth, column, traces = inside
    pairs = [*zip(outside, inside), (earth, medium.at[0:3])]
    pairs.append((wavefields.at[0], fields.at[:, :, PAD : PAD + slab, TOP : TOP + rows, :]))
    fetches = [pltpu.make_async_copy(*pair, arrived.at[n]) for n, pair in enumerate(pairs)]
    for fetch in fetches:
        fetch.start()
    clear_margins(fields, rows, range(-PAD, slab + PAD))
    clear_planes(fields, rows, beyond(slab))
    clear_margins(held, rows, range(slab))
    for fetch in fetches[:4]:
        fetch.wait()
    position = lax.axis_index("gz")
    even = position % 2 == 0

    def put(step, planes):
        inject[step] = planes

    dense_points(depth[...], column[...], traces[0], slab, rows, width, position * slab, steps, put)
    row = lax.broadcasted_iota(jnp.int32, (rows, width), 0)
    lane = lax.broadcasted_iota(jnp.int32, (rows, width), 1)
    spot = row * width + lane == source_column[0]
    for plane in range(slab):
        here = source_depth[0] == position * slab + plane
        for step in range(steps):
            amount = jnp.where(here, time_step * wavelet[0, step], 0.0)
            source[step, plane] = jnp.where(spot, amount, 0.0)
    fetches[4].wait()
    for kind in range(3):
        medium[kind] = time_step * medium[kind]
    medium[3] = 2.0 * medium[2]
    for kind in range(3):
        for far in range(2):
            at = slot(span, 0, 0) + kind * 2 + far
            above, below = medium[kind, slab - 2 + far], medium[kind, far]
            chip[at] = jnp.where(even, above, below)
            cross[at] = jnp.where(even, below, above)
    fetches[5].wait()
    run_alone(fields, held, medium, inject, source, even, chip, cross, rows, slab, span, 0)


def middle_kernel(sizes, fields_in, medium, inject, source, chip, cross,
                  fields, halo, image, next_chip, next_cross, held):
    rows, _, slab, span, _ = sizes
    flags = even, keep_low, keep_high = where_am_i()
    for kind in range(3):
        for far in range(2):
            at = slot(span, 0, 0) + kind * 2 + far
            low = jnp.where(keep_low, jnp.where(even, cross[at], chip[at]), 0.0)
            high = jnp.where(keep_high, jnp.where(even, chip[at], cross[at]), 0.0)
            halo[0, kind, far] = low
            halo[1, kind, far] = high
            if kind == 2:
                halo[0, 3, far] = 2.0 * low
                halo[1, 3, far] = 2.0 * high
    clear_margins(held, rows, range(slab))
    run_true(fields, medium, halo, inject, source, flags, chip, cross, image, True,
             rows, slab, span, 0)
    run_alone(fields, held, medium, inject, source, even, next_chip, next_cross,
              rows, slab, span, span)
    clear_planes(fields, rows, beyond(slab))


def last_kernel(sizes, fields_in, medium, halo, inject, source, chip, cross, so_far,
                fields, image):
    rows, _, slab, span, _ = sizes
    image[...] = so_far[...]
    run_true(fields, medium, halo, inject, source, where_am_i(), chip, cross, image, False,
             rows, slab, span, span)


def within(space, *arrays):
    return [pltpu.with_memory_space_constraint(a, space) for a in arrays]


def exchange(chip, cross):
    cross = swapped(cross, "gz", 1)
    chip = swapped(chip, "gz", 0)
    return chip, cross


def on_device(
    wavefields,
    earth_model,
    source_depth,
    source_column,
    wavelet,
    receiver_depth,
    receiver_column,
    traces,
):
    _, waves, _, slab, rows, width = wavefields.shape
    steps = wavelet.shape[1]
    span = slab
    assert steps == 2 * span
    sizes = (rows, width, slab, span, steps)

    vmem = pl.BlockSpec(memory_space=pltpu.VMEM)
    smem = pl.BlockSpec(memory_space=pltpu.SMEM)
    anywhere = pl.BlockSpec(memory_space=pl.ANY)

    def room(*shape):
        return pltpu.VMEM(shape, jnp.float32)

    state = room(waves, 9, slab + 2 * PAD, rows + 16, width)
    history = room(slot(span, 0, 0), rows, width)
    with_medium = room(slot(span, 0, 0) + 6, rows, width)
    dense = room(steps, slab, rows, width)
    images = room(2, slab, rows, width)
    work = waves * 9 * slab * rows * width

    def options(scale):
        return dict(
            cost_estimate=pl.CostEstimate(
                flops=scale * work, bytes_accessed=4 * work, transcendentals=0
            ),
            compiler_params=pltpu.CompilerParams(vmem_limit_bytes=LIMIT),
        )

    chip, cross, fields, medium, inject, source = pl.pallas_call(
        functools.partial(first_kernel, sizes),
        out_shape=(with_medium, with_medium, state, room(4, slab, rows, width), dense, dense),
        in_specs=[anywhere, anywhere, smem, smem] + [anywhere] * 4,
        out_specs=(vmem,) * 6,
        scratch_shapes=[
            pltpu.SMEM(wavelet.shape, jnp.float32),
            pltpu.VMEM(receiver_depth.shape, jnp.int32),
            pltpu.VMEM(receiver_column.shape, jnp.int32),
            room(*traces.shape),
            state,
            pltpu.SemaphoreType.DMA((6,)),
        ],
        name="first",
        **options(40),
    )(*within(pltpu.HBM, wavefields, earth_model), source_depth, source_column,
      *within(pltpu.HBM, wavelet, receiver_depth, receiver_column, traces))
    chip, cross = exchange(chip, cross)
    fields, halo, image, chip, cross = pl.pallas_call(
        functools.partial(middle_kernel, sizes),
        out_shape=(state, room(2, 4, 2, rows, width), images, history, history),
        in_specs=[vmem] * 6,
        out_specs=(vmem,) * 5,
        scratch_shapes=[state],
        input_output_aliases={0: 0},
        name="middle",
        **options(100),
    )(*within(pltpu.VMEM, fields, medium, inject, source, chip, cross))
    chip, cross = exchange(chip, cross)
    _, image = pl.pallas_call(
        functools.partial(last_kernel, sizes),
        out_shape=(state, images),
        in_specs=[vmem] * 8,
        out_specs=(vmem,) * 2,
        input_output_aliases={0: 0},
        name="last",
        **options(60),
    )(*within(pltpu.VMEM, fields, medium, halo, inject, source, chip, cross, image))

    total = image
    count = lax.axis_size("shot")
    for far in sorted(range(1, count), key=lambda far: -min(far, count - far)):
        total = total + cyclic(image, "shot", far)
    kind = lax.broadcasted_iota(jnp.int32, total.shape, 0)
    return total * jnp.where(kind == 0, 1.0 / (9 * steps), 1.0 / (3 * steps))


def solution(mesh):
    placed = (
        P(("parts", "shot"), None, None, "gz", None, None),
        P("parts", "gz", None, None),
        P(("parts", "shot")),
        P(("parts", "shot")),
        P(("parts", "shot"), None),
        P(("parts", "shot"), None),
        P(("parts", "shot"), None),
        P(("parts", "shot"), None, None),
    )
    return jax.shard_map(
        on_device,
        mesh=mesh,
        in_specs=placed,
        out_specs=P("parts", "gz", None, None),
        check_vma=False,
    )
```

```python
import functools

import jax
import jax.numpy as jnp
from jax import lax
from jax.experimental import pallas as pl
from jax.experimental.pallas import tpu as pltpu
from jax.sharding import PartitionSpec as P


time_step = 0.15
VX, VY, VZ, XX, YY, ZZ, XY, XZ, YZ = range(9)
PAD = 3
TOP = 8
LIMIT = 24 * 1024 * 1024


def cyclic(value, axis, steps):
    count = lax.axis_size(axis)
    return lax.ppermute(value, axis, [(s, (s + steps) % count) for s in range(count)])


def swapped(value, axis, first):
    count = lax.axis_size(axis)
    partner = {s: s for s in range(count)}
    for s in range(first, count - 1, 2):
        partner[s], partner[s + 1] = s + 1, s
    return lax.ppermute(value, axis, sorted(partner.items()))


class Fields:
    def __init__(self, ref, wave, rows):
        self.ref, self.wave, self.rows = ref, wave, rows

    def at(self, field, plane, move=0):
        return self.ref[self.wave, field, plane + PAD, TOP + move : TOP + move + self.rows, :]

    def put(self, field, plane, value):
        self.ref[self.wave, field, plane + PAD, TOP : TOP + self.rows, :] = value


def clear_margins(ref, rows, planes):
    zero = jnp.zeros((8, ref.shape[-1]), jnp.float32)
    for wave in range(2):
        for field in range(9):
            for plane in planes:
                ref[wave, field, plane + PAD, 0:TOP, :] = zero
                ref[wave, field, plane + PAD, TOP + rows : TOP + rows + 8, :] = zero


def clear_planes(ref, rows, planes):
    zero = jnp.zeros((rows, ref.shape[-1]), jnp.float32)
    for wave in range(2):
        for field in range(9):
            for plane in planes:
                ref[wave, field, plane + PAD, TOP : TOP + rows, :] = zero


def beyond(slab):
    return [*range(-PAD, 0), *range(slab, slab + PAD)]


def y_next(value):
    count = value.shape[1]
    lane = lax.broadcasted_iota(jnp.int32, value.shape, 1)
    return jnp.where(lane == count - 1, 0.0, pltpu.roll(value, count - 1, 1))


def y_last(value):
    lane = lax.broadcasted_iota(jnp.int32, value.shape, 1)
    return jnp.where(lane == 0, 0.0, pltpu.roll(value, 1, 1))


def minus(a, b):
    return a if b is None else a - b


def from_high(b, a):
    return -a if b is None else b - a


def velocity(old, new, plane, scaled, parts, low_xz, low_yz, high_zz, added=None):
    if "x" in parts:
        xx, xy, xz = old.at(XX, plane), old.at(XY, plane), old.at(XZ, plane)
        change = (old.at(XX, plane, 1) - xx) + (xy - y_last(xy)) + minus(xz, low_xz)
        new.put(VX, plane, old.at(VX, plane) + scaled * change)
    if "y" in parts:
        xy, yy, yz = old.at(XY, plane), old.at(YY, plane), old.at(YZ, plane)
        change = (xy - old.at(XY, plane, -1)) + (y_next(yy) - yy) + minus(yz, low_yz)
        new.put(VY, plane, old.at(VY, plane) + scaled * change)
    if "z" in parts:
        xz, yz, zz = old.at(XZ, plane), old.at(YZ, plane), old.at(ZZ, plane)
        change = (xz - old.at(XZ, plane, -1)) + (yz - y_last(yz)) + from_high(high_zz, zz)
        result = old.at(VZ, plane) + scaled * change
        new.put(VZ, plane, result if added is None else result + added)


def stress(old, new, plane, lam, mu, twice, low_vz, high_vx, high_vy, added=None, turn=False,
           flat=True, keep=True):
    vx, vy, vz = new.at(VX, plane), new.at(VY, plane), new.at(VZ, plane)
    e_x = vx - new.at(VX, plane, -1)
    e_y = vy - y_last(vy)
    e_z = minus(vz, low_vz)
    shared = lam * (e_x + e_y + e_z)
    if added is not None:
        shared = shared + added
    results = [(ZZ, old.at(ZZ, plane) + (shared + twice * e_z))]
    total = rotation = None
    if flat:
        xx = old.at(XX, plane) + (shared + twice * e_x)
        yy = old.at(YY, plane) + (shared + twice * e_y)
        total = xx + yy + results[0][1]
        results += [(XX, xx), (YY, yy)]
    if keep or turn:
        vx_up, vy_up = from_high(high_vx, vx), from_high(high_vy, vy)
        vz_x, vz_y = new.at(VZ, plane, 1) - vz, y_next(vz) - vz
    if flat and (keep or turn):
        vy_x, vx_y = new.at(VY, plane, 1) - vy, y_next(vx) - vx
    if keep:
        results.append((XZ, old.at(XZ, plane) + mu * (vx_up + vz_x)))
        results.append((YZ, old.at(YZ, plane) + mu * (vy_up + vz_y)))
        if flat:
            results.append((XY, old.at(XY, plane) + mu * (vx_y + vy_x)))
        for field, result in results:
            new.put(field, plane, result)
    if turn:
        rotation = (vz_y - vy_up) + (vx_up - vz_x) + (vy_x - vx_y)
    return total, rotation


def alone_parts(plane, top, left):
    near_low, near_high = plane - left, top - plane - left
    if left >= 2:
        return "xyz"
    return "".join(
        part
        for part in "xyz"
        if near_low <= (-1 if part == "z" else 0) or near_high <= (0 if part == "z" else -1)
    )


def true_parts(slab, span, done):
    moving, left = {plane: "xyz" for plane in range(slab)}, span - done
    for far in range(1, PAD):
        if done >= far and left >= far - 1:
            edge = done == far or left == far - 1
            moving[-far] = "z" if edge else "xyz"
            moving[slab - 1 + far] = "xy" if edge else "xyz"
    return moving


def slot(level, name, wave):
    return (level * 3 + name) * 2 + wave


def run_alone(first, held, medium, inject, source, even, chip, cross, rows, slab, span, start):
    for level in range(span):
        left = span - 1 - level
        for wave in range(2):
            old = Fields(first if level == 0 else held, wave, rows)
            new = Fields(held, wave, rows)
            for plane in range(slab):
                parts = alone_parts(plane, slab - 1, left)
                velocity(
                    old,
                    new,
                    plane,
                    medium[0, plane],
                    parts,
                    old.at(XZ, plane - 1) if plane else None,
                    old.at(YZ, plane - 1) if plane else None,
                    old.at(ZZ, plane + 1) if plane < slab - 1 else None,
                    inject[start + level, plane] if wave == 1 else None,
                )
            top = slab - 1
            above = (old.at(XZ, top), new.at(VZ, top), old.at(YZ, top))
            below = (old.at(ZZ, 0), new.at(VX, 0), new.at(VY, 0))
            for name in range(3):
                chip[slot(level, name, wave)] = jnp.where(even, above[name], below[name])
                cross[slot(level, name, wave)] = jnp.where(even, below[name], above[name])
            if left == 0:
                continue
            for plane in range(slab):
                if left == 1 and 0 < plane < slab - 1:
                    continue
                stress(
                    old,
                    new,
                    plane,
                    medium[1, plane],
                    medium[2, plane],
                    medium[3, plane],
                    new.at(VZ, plane - 1) if plane else None,
                    new.at(VX, plane + 1) if plane < slab - 1 else None,
                    new.at(VY, plane + 1) if plane < slab - 1 else None,
                    source[start + level, plane] if wave == 0 else None,
                    flat=alone_parts(plane, slab - 1, left - 1) != "z",
                )


def run_true(held, medium, halo, inject, source, flags, chip, cross, image, fresh,
             rows, slab, span, start, final):
    even, keep_low, keep_high = flags

    def from_below(level, name, wave):
        at = slot(level, name, wave)
        return jnp.where(keep_low, jnp.where(even, cross[at], chip[at]), 0.0)

    def from_above(level, name, wave):
        at = slot(level, name, wave)
        return jnp.where(keep_high, jnp.where(even, chip[at], cross[at]), 0.0)

    def around(kind, plane):
        if plane < 0:
            return halo[0, kind, plane + 2]
        if plane >= slab:
            return halo[1, kind, plane - slab]
        return medium[kind, plane]

    for level in range(span):
        done, left = level + 1, span - 1 - level
        moving = true_parts(slab, span, done)
        upcoming = true_parts(slab, span, done + 1) if left else moving
        for wave in range(2):
            both = Fields(held, wave, rows)
            for plane, parts in sorted(moving.items()):
                low_xz, low_yz = both.at(XZ, plane - 1), both.at(YZ, plane - 1)
                high_zz = both.at(ZZ, plane + 1)
                if plane == 0:
                    low_xz = low_xz + from_below(level, 0, wave)
                    low_yz = low_yz + from_below(level, 2, wave)
                if plane == slab - 1:
                    high_zz = high_zz + from_above(level, 0, wave)
                own = 0 <= plane < slab
                velocity(
                    both,
                    both,
                    plane,
                    around(0, plane),
                    parts,
                    low_xz,
                    low_yz,
                    high_zz,
                    inject[start + level, plane] if own and wave == 1 else None,
                )
        shaking = list(range(slab))
        for far in range(1, PAD):
            if done >= far and left >= far:
                shaking += [-far, slab - 1 + far]
        for plane in sorted(shaking):
            own = 0 <= plane < slab
            found = []
            for wave in range(2):
                both = Fields(held, wave, rows)
                low_vz = both.at(VZ, plane - 1)
                high_vx, high_vy = both.at(VX, plane + 1), both.at(VY, plane + 1)
                if plane == 0:
                    low_vz = low_vz + from_below(level, 1, wave)
                if plane == slab - 1:
                    high_vx = high_vx + from_above(level, 1, wave)
                    high_vy = high_vy + from_above(level, 2, wave)
                found.append(
                    stress(
                        both,
                        both,
                        plane,
                        around(1, plane),
                        around(2, plane),
                        around(3, plane),
                        low_vz,
                        high_vx,
                        high_vy,
                        source[start + level, plane] if own and wave == 0 else None,
                        turn=own and wave == 1,
                        flat=own or upcoming[plane] != "z",
                        keep=left > 0 or not final,
                    )
                )
            if own:
                (given, _), (taken, rotation) = found
                if fresh and level == 0:
                    image[0, plane] = given * taken
                    image[1, plane] = given * rotation
                else:
                    image[0, plane] += given * taken
                    image[1, plane] += given * rotation


def where_am_i():
    position = lax.axis_index("gz")
    return position % 2 == 0, position > 0, position < lax.axis_size("gz") - 1


def dense_points(depth, column, amounts, slab, rows, width, offset, steps, put):
    points = depth.shape[1]
    row = (depth - offset) * rows + column // width
    where = lax.broadcasted_iota(jnp.int32, (width, points), 0) == column % width
    where = where.astype(jnp.bfloat16)
    where = jnp.concatenate([where, where, where], axis=1)
    which = lax.broadcasted_iota(jnp.int32, (slab * rows, points), 0) == row
    for step in range(steps):
        whole = jnp.where(which, time_step * amounts[step : step + 1, :], 0.0)
        high = whole.astype(jnp.bfloat16)
        rest = whole - high.astype(jnp.float32)
        middle = rest.astype(jnp.bfloat16)
        low = (rest - middle.astype(jnp.float32)).astype(jnp.bfloat16)
        planes = lax.dot_general(
            jnp.concatenate([high, middle, low], axis=1),
            where,
            (((1,), (1,)), ((), ())),
            preferred_element_type=jnp.float32,
        )
        put(step, planes.reshape(slab, rows, width))


def first_kernel(sizes, wavefields, earth, *refs):
    rows, width, slab, span, steps = sizes
    scalars, outside, results, inside = refs[:2], refs[2:6], refs[6:12], refs[12:16]
    held, arrived = refs[16:]
    chip, cross, fields, medium, inject, source = results
    source_depth, source_column = scalars
    wavelet, depth, column, traces = inside
    pairs = [*zip(outside, inside), (earth, medium.at[0:3])]
    pairs.append((wavefields.at[0], fields.at[:, :, PAD : PAD + slab, TOP : TOP + rows, :]))
    fetches = [pltpu.make_async_copy(*pair, arrived.at[n]) for n, pair in enumerate(pairs)]
    for fetch in fetches:
        fetch.start()
    clear_margins(fields, rows, range(-PAD, slab + PAD))
    clear_planes(fields, rows, beyond(slab))
    clear_margins(held, rows, range(slab))
    for fetch in fetches[:4]:
        fetch.wait()
    position = lax.axis_index("gz")
    even = position % 2 == 0

    def put(step, planes):
        inject[step] = planes

    dense_points(depth[...], column[...], traces[0], slab, rows, width, position * slab, steps, put)
    row = lax.broadcasted_iota(jnp.int32, (rows, width), 0)
    lane = lax.broadcasted_iota(jnp.int32, (rows, width), 1)
    spot = row * width + lane == source_column[0]
    for plane in range(slab):
        here = source_depth[0] == position * slab + plane
        for step in range(steps):
            amount = jnp.where(here, time_step * wavelet[0, step], 0.0)
            source[step, plane] = jnp.where(spot, amount, 0.0)
    fetches[4].wait()
    for kind in range(3):
        medium[kind] = time_step * medium[kind]
    medium[3] = 2.0 * medium[2]
    for kind in range(3):
        for far in range(2):
            at = slot(span, 0, 0) + kind * 2 + far
            above, below = medium[kind, slab - 2 + far], medium[kind, far]
            chip[at] = jnp.where(even, above, below)
            cross[at] = jnp.where(even, below, above)
    fetches[5].wait()
    run_alone(fields, held, medium, inject, source, even, chip, cross, rows, slab, span, 0)


def middle_kernel(sizes, fields_in, medium, inject, source, chip, cross,
                  fields, halo, image, next_chip, next_cross, held):
    rows, _, slab, span, _ = sizes
    flags = even, keep_low, keep_high = where_am_i()
    for kind in range(3):
        for far in range(2):
            at = slot(span, 0, 0) + kind * 2 + far
            low = jnp.where(keep_low, jnp.where(even, cross[at], chip[at]), 0.0)
            high = jnp.where(keep_high, jnp.where(even, chip[at], cross[at]), 0.0)
            halo[0, kind, far] = low
            halo[1, kind, far] = high
            if kind == 2:
                halo[0, 3, far] = 2.0 * low
                halo[1, 3, far] = 2.0 * high
    clear_margins(held, rows, range(slab))
    run_true(fields, medium, halo, inject, source, flags, chip, cross, image, True,
             rows, slab, span, 0, False)
    run_alone(fields, held, medium, inject, source, even, next_chip, next_cross,
              rows, slab, span, span)
    clear_planes(fields, rows, beyond(slab))


def last_kernel(sizes, fields_in, medium, halo, inject, source, chip, cross, so_far,
                fields, image):
    rows, _, slab, span, _ = sizes
    image[...] = so_far[...]
    run_true(fields, medium, halo, inject, source, where_am_i(), chip, cross, image, False,
             rows, slab, span, span, True)


def within(space, *arrays):
    return [pltpu.with_memory_space_constraint(a, space) for a in arrays]


def exchange(chip, cross):
    cross = swapped(cross, "gz", 1)
    chip = swapped(chip, "gz", 0)
    return chip, cross


def on_device(
    wavefields,
    earth_model,
    source_depth,
    source_column,
    wavelet,
    receiver_depth,
    receiver_column,
    traces,
):
    _, waves, _, slab, rows, width = wavefields.shape
    steps = wavelet.shape[1]
    span = slab
    assert steps == 2 * span
    sizes = (rows, width, slab, span, steps)

    vmem = pl.BlockSpec(memory_space=pltpu.VMEM)
    smem = pl.BlockSpec(memory_space=pltpu.SMEM)
    anywhere = pl.BlockSpec(memory_space=pl.ANY)

    def room(*shape):
        return pltpu.VMEM(shape, jnp.float32)

    state = room(waves, 9, slab + 2 * PAD, rows + 16, width)
    history = room(slot(span, 0, 0), rows, width)
    with_medium = room(slot(span, 0, 0) + 6, rows, width)
    dense = room(steps, slab, rows, width)
    images = room(2, slab, rows, width)
    work = waves * 9 * slab * rows * width

    def options(scale):
        return dict(
            cost_estimate=pl.CostEstimate(
                flops=scale * work, bytes_accessed=4 * work, transcendentals=0
            ),
            compiler_params=pltpu.CompilerParams(vmem_limit_bytes=LIMIT),
        )

    chip, cross, fields, medium, inject, source = pl.pallas_call(
        functools.partial(first_kernel, sizes),
        out_shape=(with_medium, with_medium, state, room(4, slab, rows, width), dense, dense),
        in_specs=[anywhere, anywhere, smem, smem] + [anywhere] * 4,
        out_specs=(vmem,) * 6,
        scratch_shapes=[
            pltpu.SMEM(wavelet.shape, jnp.float32),
            pltpu.VMEM(receiver_depth.shape, jnp.int32),
            pltpu.VMEM(receiver_column.shape, jnp.int32),
            room(*traces.shape),
            state,
            pltpu.SemaphoreType.DMA((6,)),
        ],
        name="first",
        **options(40),
    )(*within(pltpu.HBM, wavefields, earth_model), source_depth, source_column,
      *within(pltpu.HBM, wavelet, receiver_depth, receiver_column, traces))
    chip, cross = exchange(chip, cross)
    fields, halo, image, chip, cross = pl.pallas_call(
        functools.partial(middle_kernel, sizes),
        out_shape=(state, room(2, 4, 2, rows, width), images, history, history),
        in_specs=[vmem] * 6,
        out_specs=(vmem,) * 5,
        scratch_shapes=[state],
        input_output_aliases={0: 0},
        name="middle",
        **options(100),
    )(*within(pltpu.VMEM, fields, medium, inject, source, chip, cross))
    chip, cross = exchange(chip, cross)
    _, image = pl.pallas_call(
        functools.partial(last_kernel, sizes),
        out_shape=(state, images),
        in_specs=[vmem] * 8,
        out_specs=(vmem,) * 2,
        input_output_aliases={0: 0},
        name="last",
        **options(60),
    )(*within(pltpu.VMEM, fields, medium, halo, inject, source, chip, cross, image))

    total = image
    count = lax.axis_size("shot")
    for far in sorted(range(1, count), key=lambda far: -min(far, count - far)):
        total = total + cyclic(image, "shot", far)
    kind = lax.broadcasted_iota(jnp.int32, total.shape, 0)
    return total * jnp.where(kind == 0, 1.0 / (9 * steps), 1.0 / (3 * steps))


def solution(mesh):
    placed = (
        P(("parts", "shot"), None, None, "gz", None, None),
        P("parts", "gz", None, None),
        P(("parts", "shot")),
        P(("parts", "shot")),
        P(("parts", "shot"), None),
        P(("parts", "shot"), None),
        P(("parts", "shot"), None),
        P(("parts", "shot"), None, None),
    )
    return jax.shard_map(
        on_device,
        mesh=mesh,
        in_specs=placed,
        out_specs=P("parts", "gz", None, None),
        check_vma=False,
    )
```
